32 devices in a mesh: grp: 4 (over z), tm: 8 (over y, x, core).
Axes of the slice: x: 2, y: 2, z: 4, core: 2. Of those that a mesh axis runs over, the one named last changes fastest.
Arguments:
- initial: float32 [8, 16384], P('grp'), parts along dimension 0, may hold values from -1 to 1
- forcing: float32 [8, 32, 16384], P('grp', 'tm'), parts along dimension 0, may hold values from -1.8 to 1.8
- fine_blocks: float32 [16, 3, 128, 128], replicated, may hold values from -0.2 to 0.9, as said below
- coarse_blocks: float32 [16, 3, 128, 128], replicated, may hold values from -0.2 to 0.9, as said below
Outputs:
- solution: float32 [8, 32, 16384], P('grp', 'tm'), parts along dimension 0
The draws below stay inside these ranges and needn't reach their ends.
There are 4 independent parts, one for each index of `grp`. The reference program is written for one: setup_inputs(seed, part) draws one part's arguments, and reference() takes and returns one part's arrays. A program takes and returns all parts, laid end to end along the dimension named above; an argument that names none is the same for every part. Nothing has to cross between parts.
Inputs may be any that keep to these rules, and one draw needn't show every extreme that they name: `fine_blocks`: 16 x 3 blocks of 128 x 128. `coarse_blocks`: 16 x 3 blocks of 128 x 128.
All inputs are finite; a program needn't handle non-finite values.
Results may differ from the reference program's by a relative error of at most 0.00013.
Values sent between devices are 32-bit elements; how exact they have to be, the bound alone decides.
A program may use at most 64 MiB of HBM per device.

```python
import math
import jax
import jax.numpy as jnp
from jax import lax

W = 16384
BLK = 128
ZONES = 16
INST = 2
M = 4
ITERS = 1
NT = 32


def make_blocks(key, centre):
    noise = jnp.clip(jax.random.normal(key, (ZONES, 3, BLK, BLK), jnp.float32), -4.0, 4.0)
    noise = noise / math.sqrt(BLK)
    weights = jnp.array([0.12, 0.25, 0.12], jnp.float32)[None, :, None, None]
    middle = jnp.array([0.0, 1.0, 0.0], jnp.float32)[None, :, None, None]
    return noise * weights + centre * middle * jnp.eye(BLK, dtype=jnp.float32)[None, None]


def draw_fine_blocks(key, part):
    return make_blocks(jax.random.fold_in(key, 11), 0.7)


def draw_coarse_blocks(key, part):
    return make_blocks(jax.random.fold_in(key, 23), 0.65)


def levels(stream_key, shape, split, low, top_value):
    gain = 1.0
    for position, parts in split:
        steps = jax.random.uniform(jax.random.fold_in(jax.random.fold_in(stream_key, 6), position), (parts,), jnp.float32, low / len(split), top_value / len(split))
        gain = gain * jnp.repeat(jnp.exp(steps), shape[position] // parts).reshape((-1,) + (1,) * (len(shape) - 1 - position))
    return gain


def normal_values(rng, extent, deviation, reach, pieces=(), kind=jnp.bfloat16):
    gain = levels(rng, extent, pieces, -0.22, 0.18) if pieces else 1.0
    values = jax.random.normal(rng, extent, jnp.float32) * deviation * gain
    return jnp.minimum(jnp.maximum(values, -reach), reach).astype(kind)


def setup_inputs(seed: int = 0, part: int = 0) -> dict:
    streams_of = jax.random.split(jax.random.key(seed), 5)
    own_keys = jax.random.split(jax.random.fold_in(streams_of[4], part), 5)
    initial = jnp.clip(jax.random.uniform(own_keys[0], (INST, W), jnp.float32, -1.0, 1.0), -1.0, 1.0)
    forcing = normal_values(own_keys[1], (INST, NT, W), 0.3, 1.8, ((1, 8),), jnp.float32)
    fine_blocks = draw_fine_blocks(jax.random.fold_in(streams_of[4], 71), part)
    coarse_blocks = draw_coarse_blocks(jax.random.fold_in(streams_of[4], 71), part)
    return {"initial": initial, "forcing": forcing, "fine_blocks": fine_blocks, "coarse_blocks": coarse_blocks}


DELTA = 0.05


def propagate(states, blocks, delta_t):
    layout = states.shape
    block_size = blocks.shape[-1]
    zone_count = blocks.shape[0]
    grouped = states.reshape(-1, layout[-1] // block_size, block_size)
    border = jnp.zeros_like(grouped[:, :1])
    left_side = jnp.concatenate([border, grouped[:, :-1]], axis=1)
    right_side = jnp.concatenate([grouped[:, 1:], border], axis=1)
    stacked = jnp.stack([left_side, grouped, right_side]).reshape(3, grouped.shape[0], -1, zone_count, block_size)
    mixing = jnp.einsum("kbrzn,zkmn->brzm", stacked, blocks, precision=lax.Precision.HIGHEST).reshape(layout)
    solved = mixing
    for _ in range(2):
        cubed_part = solved * solved * solved
        solved = solved - (solved - delta_t * (solved - cubed_part) - mixing) / (1.0 - delta_t + 3.0 * delta_t * solved * solved)
    return solved


def sweep(current, forcing_grid, carried, blocks, want_next):
    running = carried
    columns = []
    for slot in range(current.shape[2] - 1):
        running = propagate(running, blocks, DELTA) + forcing_grid[:, :, slot]
        columns.append(running)
    columns.append(current[:, :, -1])
    updated = jnp.stack(columns, axis=2)
    following = propagate(running, blocks, DELTA) + forcing_grid[:, :, -1] if want_next else None
    return updated, following


def coarse_chain(start, rhs_values, blocks, coarse_dt):
    def advance(carry_state, source):
        stepped = propagate(carry_state, blocks, coarse_dt) + source
        return stepped, stepped
    _, history = lax.scan(advance, start, jnp.moveaxis(rhs_values, 1, 0))
    return jnp.moveaxis(history, 0, 1)


def reference(initial, forcing, fine_blocks, coarse_blocks):
    members = forcing.shape[0]
    grid_cells = forcing.shape[2]
    forcing_grid = forcing.reshape(members, -1, M, grid_cells)
    current = jnp.zeros(forcing_grid.shape, jnp.float32)

    def carried_in(values):
        return jnp.concatenate([initial[:, None], values[:, :-1, -1]], axis=1)

    current, _ = sweep(current, forcing_grid, carried_in(current), fine_blocks, False)
    for _ in range(ITERS):
        corner = propagate(current[:, :, -2], fine_blocks, DELTA) + forcing_grid[:, :, -1]
        current = jnp.concatenate([current[:, :, :-1], corner[:, :, None]], axis=2)
        carried = carried_in(current)
        current, following = sweep(current, forcing_grid, carried, fine_blocks, True)
        coarse_rhs = following - propagate(carried, coarse_blocks, DELTA * M)
        coarse_vals = coarse_chain(initial, coarse_rhs, coarse_blocks, DELTA * M)
        current = jnp.concatenate([current[:, :, :-1], coarse_vals[:, :, None]], axis=2)
        current, _ = sweep(current, forcing_grid, carried_in(current), fine_blocks, False)
    return current.reshape(members, -1, grid_cells)
```

```python
import functools

import jax
import jax.numpy as jnp
from jax import lax
from jax.experimental import pallas as pl
from jax.experimental.pallas import tpu as pltpu
from jax.sharding import PartitionSpec as P

M = 4
DELTA = 0.05
MESH = pl.DeviceIdType.MESH


def newton(mixing, delta_t):
    solved = mixing
    for _ in range(2):
        squared = solved * solved
        solved = (mixing + (2.0 * delta_t) * solved * squared) / (
            (1.0 - delta_t) + (3.0 * delta_t) * squared
        )
    return solved


def kernel(
    n, inst, zones, reps,
    init_ref, forc_ref, fine_ref, coarse_ref, out_ref,
    raw, weights, x, ubuf, carr, rbuf, pbuf, qbuf, gbuf,
    load_sem, carr_send, carr_recv, r_send, r_recv,
):
    me = lax.axis_index("tm")
    blk = raw.shape[-1]
    rows = inst * reps
    coarse_dt = DELTA * M

    loads = [pltpu.make_async_copy(ref, raw.at[w], load_sem.at[w]) for w, ref in enumerate((fine_ref, coarse_ref))]
    for load in loads:
        load.start()

    barrier = pltpu.get_barrier_semaphore()
    for step in range(1, n):
        pl.semaphore_signal(barrier, inc=1, device_id={"tm": lax.rem(me + step, n)}, device_id_type=MESH)

    def initial_at(z):
        return jnp.concatenate(
            [init_ref[pl.ds(z * inst + i, reps, stride=zones * inst), :] for i in range(inst)], axis=0
        )

    def forcing_at(slot, z):
        return jnp.concatenate(
            [forc_ref[pl.ds((i * reps * zones + z) * M + slot, reps, stride=zones * M), :] for i in range(inst)],
            axis=0,
        )

    def emit_out(slot, z, value):
        for i in range(inst):
            out_ref[pl.ds((i * reps * zones + z) * M + slot, reps, stride=zones * M), :] = value[
                i * reps : (i + 1) * reps
            ]

    row = lax.broadcasted_iota(jnp.int32, (rows, blk), 0)

    def put(dst, z, value):
        def write(slot, v):
            high = v.astype(jnp.bfloat16)
            low = (v - high.astype(jnp.float32)).astype(jnp.bfloat16)
            x[dst, slot, :rows] = high
            x[dst, slot, rows:] = low

        write(z + 1, value)
        if z == 0:
            rolled = pltpu.roll(value, rows - 1, 0)
            write(zones + 1, jnp.where(row % reps == reps - 1, 0.0, rolled))
        if z == zones - 1:
            rolled = pltpu.roll(value, 1, 0)
            write(0, jnp.where(row % reps == 0, 0.0, rolled))

    def propagate(src, which, delta_t, emit):
        for z in range(zones):
            left = jnp.concatenate([x[src, z + k] for k in range(3)], axis=1)
            acc = jnp.dot(left, weights[which, z], preferred_element_type=jnp.float32)
            mixing = (acc[:rows, :blk] + acc[:rows, blk:]) + (acc[rows:, :blk] + acc[rows:, blk:])
            emit(z, newton(mixing, delta_t))

    def prepare(which):
        loads[which].wait()

        @pl.loop(0, zones)
        def _(z):
            for k in range(3):
                turned = raw[which, z, k].T
                high = turned.astype(jnp.bfloat16)
                weights[which, z, k * blk : (k + 1) * blk, :blk] = high
                weights[which, z, k * blk : (k + 1) * blk, blk:] = (
                    turned - high.astype(jnp.float32)
                ).astype(jnp.bfloat16)

    def fine_steps(first, last, sink):
        def body(t, _):
            p = lax.rem(t, 2)

            def emit(z, s):
                value = s + forcing_at(t, z)
                put(1 - p, z, value)
                sink(t, z, value)

            propagate(p, 0, DELTA, emit)
            return 0

        lax.fori_loop(first, last, body, 0)

    def store_to(buf):
        def emit(z, value):
            buf[z] = value

        return emit

    prepare(0)
    for z in range(zones):
        put(0, z, initial_at(z))
        put(1, z, forcing_at(0, z))
    fine_steps(jnp.where(me == 0, 0, 1), M, lambda t, z, v: store_to(ubuf)(z, v))
    pl.semaphore_wait(barrier, n - 1)

    onward = pltpu.make_async_remote_copy(
        src_ref=ubuf, dst_ref=carr, send_sem=carr_send, recv_sem=carr_recv,
        device_id={"tm": lax.rem(me + 1, n)}, device_id_type=MESH,
    )

    @pl.when(me < n - 1)
    def _():
        onward.start()

    prepare(1)
    for z in range(zones):
        put(0, z, initial_at(z))
    propagate(0, 1, coarse_dt, store_to(pbuf))

    @pl.when(me == 0)
    def _():
        for z in range(zones):
            rbuf[0, z] = ubuf[z] - pbuf[z]

    @pl.when(me > 0)
    def _():
        onward.wait_recv()
        for z in range(zones):
            put(0, z, carr[z])
        propagate(0, 1, coarse_dt, store_to(qbuf))
        fine_steps(0, M, lambda t, z, v: store_to(gbuf)(z, v))
        for z in range(zones):
            rbuf[me, z] = gbuf[z] - qbuf[z]

    def share(step):
        return pltpu.make_async_remote_copy(
            src_ref=rbuf.at[me], dst_ref=rbuf.at[me], send_sem=r_send.at[step], recv_sem=r_recv.at[me],
            device_id={"tm": lax.rem(me + step, n)}, device_id_type=MESH,
        )

    for step in range(n - 1, 0, -1):

        @pl.when(me + step < n)
        def _():
            share(step).start()

    def chain(j, _):
        pltpu.make_async_remote_copy(
            src_ref=rbuf.at[j], dst_ref=rbuf.at[j], send_sem=r_send.at[0], recv_sem=r_recv.at[j],
            device_id={"tm": lax.rem(me + 1, n)}, device_id_type=MESH,
        ).wait_recv()
        for z in range(zones):
            put(0, z, pbuf[z] + rbuf[j, z])
        propagate(0, 1, coarse_dt, store_to(pbuf))
        return 0

    lax.fori_loop(0, me, chain, 0)
    for z in range(zones):
        emit_out(M - 1, z, pbuf[z] + rbuf[me, z])
    fine_steps(0, M - 1, emit_out)

    @pl.when(me < n - 1)
    def _():
        onward.wait_send()

    for step in range(n - 1, 0, -1):

        @pl.when(me + step < n)
        def _():
            share(step).wait_send()


def solution(mesh):
    n = mesh.shape["tm"]

    def body(initial, forcing, fine_blocks, coarse_blocks):
        inst, slots, cells = forcing.shape
        zones, _, blk, _ = fine_blocks.shape
        blocks = cells // blk
        reps = blocks // zones
        rows = inst * reps
        assert slots == M
        init_rows = initial.reshape(inst, blocks, blk).transpose(1, 0, 2).reshape(-1, blk)
        forc_rows = forcing.reshape(inst, slots, blocks, blk).transpose(0, 2, 1, 3).reshape(-1, blk)
        state = pltpu.VMEM((zones, rows, blk), jnp.float32)
        out = pl.pallas_call(
            functools.partial(kernel, n, inst, zones, reps),
            out_shape=jax.ShapeDtypeStruct(forc_rows.shape, jnp.float32),
            in_specs=[pl.BlockSpec(memory_space=pltpu.VMEM)] * 2 + [pl.BlockSpec(memory_space=pl.ANY)] * 2,
            out_specs=pl.BlockSpec(memory_space=pltpu.VMEM),
            scratch_shapes=[
                pltpu.VMEM((2,) + fine_blocks.shape, jnp.float32),
                pltpu.VMEM((2, zones, 3 * blk, 2 * blk), jnp.bfloat16),
                pltpu.VMEM((2, zones + 2, 2 * rows, blk), jnp.bfloat16),
                state,
                state,
                pltpu.VMEM((n, zones, rows, blk), jnp.float32),
                state,
                state,
                state,
                pltpu.SemaphoreType.DMA((2,)),
                pltpu.SemaphoreType.DMA,
                pltpu.SemaphoreType.DMA,
                pltpu.SemaphoreType.DMA((n,)),
                pltpu.SemaphoreType.DMA((n,)),
            ],
            compiler_params=pltpu.CompilerParams(collective_id=0, has_side_effects=True),
        )(init_rows, forc_rows, fine_blocks, coarse_blocks)
        return out.reshape(inst, blocks, slots, blk).transpose(0, 2, 1, 3).reshape(forcing.shape)

    in_specs = (P("grp", None), P("grp", "tm", None), P(), P())
    out_specs = P("grp", "tm", None)
    return jax.shard_map(body, mesh=mesh, in_specs=in_specs, out_specs=out_specs, check_vma=False)
```

```python
import functools

import jax
import jax.numpy as jnp
from jax import lax
from jax.experimental import pallas as pl
from jax.experimental.pallas import tpu as pltpu
from jax.sharding import PartitionSpec as P

M = 4
DELTA = 0.05
MESH = pl.DeviceIdType.MESH


def newton(mixing, delta_t):
    solved = mixing
    for _ in range(2):
        squared = solved * solved
        solved = (mixing + (2.0 * delta_t) * solved * squared) / (
            (1.0 - delta_t) + (3.0 * delta_t) * squared
        )
    return solved


def kernel(
    n, inst, zones, reps, pieces,
    init_hbm, forc_hbm, fine_hbm, coarse_hbm, out_ref,
    init_ref, forc_ref, raw, weights, x, ubuf, carr, rbuf, pbuf, qbuf,
    load_sem, state_sem, carr_send, carr_recv, r_send, r_recv, fwd_send,
):
    me = lax.axis_index("tm")
    blk = raw.shape[-1]
    rows = inst * reps
    coarse_dt = DELTA * M
    part = zones // pieces
    odd = lax.rem(me, 2)

    def load(which, c):
        span = pl.ds(c * part, part)
        return pltpu.make_async_copy((fine_hbm, coarse_hbm)[which].at[span], raw.at[which, span], load_sem.at[which, c])

    state_loads = [
        pltpu.make_async_copy(init_hbm, init_ref, state_sem.at[0]),
        pltpu.make_async_copy(forc_hbm, forc_ref, state_sem.at[1]),
    ]
    for c in range(pieces):
        load(0, c).start()
    for copy in state_loads:
        copy.start()

    barrier = pltpu.get_barrier_semaphore()
    for step in range(1, n):
        pl.semaphore_signal(barrier, inc=1, device_id={"tm": lax.rem(me + step, n)}, device_id_type=MESH)

    def initial_at(z):
        return jnp.concatenate(
            [init_ref[pl.ds(z * inst + i, reps, stride=zones * inst), :] for i in range(inst)], axis=0
        )

    def forcing_at(slot, z):
        return jnp.concatenate(
            [forc_ref[pl.ds((i * reps * zones + z) * M + slot, reps, stride=zones * M), :] for i in range(inst)],
            axis=0,
        )

    def emit_out(slot, z, value):
        for i in range(inst):
            out_ref[pl.ds((i * reps * zones + z) * M + slot, reps, stride=zones * M), :] = value[
                i * reps : (i + 1) * reps
            ]

    row = lax.broadcasted_iota(jnp.int32, (rows, blk), 0)

    def put(dst, z, value):
        def write(slot, v):
            high = v.astype(jnp.bfloat16)
            low = (v - high.astype(jnp.float32)).astype(jnp.bfloat16)
            x[dst, slot, :rows] = high
            x[dst, slot, rows:] = low

        write(z + 1, value)
        if z == 0:
            rolled = pltpu.roll(value, rows - 1, 0)
            write(zones + 1, jnp.where(row % reps == reps - 1, 0.0, rolled))
        if z == zones - 1:
            rolled = pltpu.roll(value, 1, 0)
            write(0, jnp.where(row % reps == 0, 0.0, rolled))

    def propagate(src, which, delta_t, emit):
        for z in range(zones):
            left = jnp.concatenate([x[src, z + k] for k in range(3)], axis=1)
            acc = jnp.dot(left, weights[which, z], preferred_element_type=jnp.float32)
            mixing = (acc[:rows, :blk] + acc[:rows, blk:]) + (acc[rows:, :blk] + acc[rows:, blk:])
            emit(z, newton(mixing, delta_t))

    def prepare(which):
        @pl.loop(0, pieces)
        def _(c):
            load(which, c).wait()
            for zz in range(part):
                z = c * part + zz
                for k in range(3):
                    turned = raw[which, z, k].T
                    high = turned.astype(jnp.bfloat16)
                    weights[which, z, k * blk : (k + 1) * blk, :blk] = high
                    weights[which, z, k * blk : (k + 1) * blk, blk:] = (
                        turned - high.astype(jnp.float32)
                    ).astype(jnp.bfloat16)

    def fine_step(t, src, sink, keep=True):
        def emit(z, s):
            value = s + forcing_at(t, z)
            if keep:
                put(1 - src, z, value)
            sink(z, value)

        propagate(src, 0, DELTA, emit)

    def store_to(buf):
        def emit(z, value):
            buf[z] = value

        return emit

    def drop(z, value):
        pass

    prepare(0)
    for c in range(pieces):
        load(1, c).start()
    for copy in state_loads:
        copy.wait()

    @pl.when(me == 0)
    def _():
        for z in range(zones):
            put(0, z, initial_at(z))
        fine_step(0, 0, drop)

    @pl.when(me > 0)
    def _():
        for z in range(zones):
            put(1, z, forcing_at(0, z))

    for t in range(1, M):
        fine_step(t, t % 2, store_to(ubuf) if t == M - 1 else drop, keep=t < M - 1)
    pl.semaphore_wait(barrier, n - 1)

    onward = pltpu.make_async_remote_copy(
        src_ref=ubuf, dst_ref=carr, send_sem=carr_send, recv_sem=carr_recv,
        device_id={"tm": lax.rem(me + 1, n)}, device_id_type=MESH,
    )

    @pl.when(me < n - 1)
    def _():
        onward.start()

    prepare(1)
    for z in range(zones):
        put(0, z, initial_at(z))
    propagate(0, 1, coarse_dt, store_to(pbuf))

    @pl.when(me == 0)
    def _():
        for z in range(zones):
            rbuf[0, z] = ubuf[z] - pbuf[z]

    @pl.when(me > 0)
    def _():
        onward.wait_recv()
        for z in range(zones):
            put(0, z, carr[z])
        propagate(0, 1, coarse_dt, store_to(qbuf))
        for t in range(M - 1):
            fine_step(t, t % 2, drop)

        def right_side(z, value):
            rbuf[me, z] = value - qbuf[z]

        fine_step(M - 1, (M - 1) % 2, right_side, keep=False)

    def share(target):
        return pltpu.make_async_remote_copy(
            src_ref=rbuf.at[me], dst_ref=rbuf.at[me], send_sem=r_send.at[target], recv_sem=r_recv.at[me],
            device_id={"tm": target}, device_id_type=MESH,
        )

    def forward(j):
        return pltpu.make_async_remote_copy(
            src_ref=rbuf.at[j], dst_ref=rbuf.at[j], send_sem=fwd_send.at[j], recv_sem=r_recv.at[j],
            device_id={"tm": lax.rem(me + n - 1, n)}, device_id_type=MESH,
        )

    for target in range(n - 1, 0, -2):

        @pl.when(me < target)
        def _():
            share(target).start()

    def chain(j, _):
        forward(j).wait_recv()

        @pl.when(jnp.logical_and(odd == 1, j < me - 1))
        def _():
            forward(j).start()

        for z in range(zones):
            put(0, z, pbuf[z] + rbuf[j, z])
        propagate(0, 1, coarse_dt, store_to(pbuf))
        return 0

    lax.fori_loop(0, me, chain, 0)
    for z in range(zones):
        emit_out(M - 1, z, pbuf[z] + rbuf[me, z])
    for t in range(M - 1):
        fine_step(t, t % 2, functools.partial(emit_out, t), keep=t < M - 2)

    @pl.when(me < n - 1)
    def _():
        onward.wait_send()

    for target in range(n - 1, 0, -2):

        @pl.when(me < target)
        def _():
            share(target).wait_send()

    def drain(j, _):
        forward(j).wait_send()
        return 0

    lax.fori_loop(0, jnp.where(odd == 1, me - 1, 0), drain, 0)


def solution(mesh):
    n = mesh.shape["tm"]

    def body(initial, forcing, fine_blocks, coarse_blocks):
        inst, slots, cells = forcing.shape
        zones, _, blk, _ = fine_blocks.shape
        blocks = cells // blk
        reps = blocks // zones
        rows = inst * reps
        assert slots == M and n % 2 == 0
        pieces = 4 if zones % 4 == 0 else 1
        init_rows = initial.reshape(inst, blocks, blk).transpose(1, 0, 2).reshape(-1, blk)
        forc_rows = forcing.reshape(inst, slots, blocks, blk).transpose(0, 2, 1, 3).reshape(-1, blk)
        state = pltpu.VMEM((zones, rows, blk), jnp.float32)
        out = pl.pallas_call(
            functools.partial(kernel, n, inst, zones, reps, pieces),
            out_shape=jax.ShapeDtypeStruct(forc_rows.shape, jnp.float32),
            in_specs=[pl.BlockSpec(memory_space=pl.ANY)] * 4,
            out_specs=pl.BlockSpec(memory_space=pltpu.VMEM),
            scratch_shapes=[
                pltpu.VMEM(init_rows.shape, jnp.float32),
                pltpu.VMEM(forc_rows.shape, jnp.float32),
                pltpu.VMEM((2,) + fine_blocks.shape, jnp.float32),
                pltpu.VMEM((2, zones, 3 * blk, 2 * blk), jnp.bfloat16),
                pltpu.VMEM((2, zones + 2, 2 * rows, blk), jnp.bfloat16),
                state,
                state,
                pltpu.VMEM((n, zones, rows, blk), jnp.float32),
                state,
                state,
                pltpu.SemaphoreType.DMA((2, pieces)),
                pltpu.SemaphoreType.DMA((2,)),
                pltpu.SemaphoreType.DMA,
                pltpu.SemaphoreType.DMA,
                pltpu.SemaphoreType.DMA((n,)),
                pltpu.SemaphoreType.DMA((n,)),
                pltpu.SemaphoreType.DMA((n,)),
            ],
            compiler_params=pltpu.CompilerParams(collective_id=0, has_side_effects=True),
        )(init_rows, forc_rows, fine_blocks, coarse_blocks)
        return out.reshape(inst, blocks, slots, blk).transpose(0, 2, 1, 3).reshape(forcing.shape)

    in_specs = (P("grp", None), P("grp", "tm", None), P(), P())
    out_specs = P("grp", "tm", None)
    return jax.shard_map(body, mesh=mesh, in_specs=in_specs, out_specs=out_specs, check_vma=False)
```

```python
import functools

import jax
import jax.numpy as jnp
from jax import lax
from jax.experimental import pallas as pl
from jax.experimental.pallas import tpu as pltpu
from jax.sharding import PartitionSpec as P

M = 4
DELTA = 0.05
MESH = pl.DeviceIdType.MESH


def newton(mixing, delta_t):
    solved = mixing
    for _ in range(2):
        squared = solved * solved
        solved = (mixing + (2.0 * delta_t) * solved * squared) / (
            (1.0 - delta_t) + (3.0 * delta_t) * squared
        )
    return solved


def kernel(
    n, inst, zones, reps, pieces,
    init_hbm, forc_hbm, fine_hbm, coarse_hbm, out_ref,
    init_ref, forc_ref, raw, weights, x, ubuf, carr, rbuf, pbuf, qbuf,
    load_sem, state_sem, carr_send, carr_recv, r_send, r_recv, fwd_send,
):
    me = lax.axis_index("tm")
    blk = raw.shape[-1]
    rows = inst * reps
    coarse_dt = DELTA * M
    part = zones // pieces
    odd = lax.rem(me, 2)

    def load(which, c):
        span = pl.ds(c * part, part)
        return pltpu.make_async_copy((fine_hbm, coarse_hbm)[which].at[span], raw.at[which, span], load_sem.at[which, c])

    state_loads = [
        pltpu.make_async_copy(init_hbm, init_ref, state_sem.at[0]),
        pltpu.make_async_copy(forc_hbm, forc_ref, state_sem.at[1]),
    ]
    for c in range(pieces):
        load(0, c).start()
    for copy in state_loads:
        copy.start()

    barrier = pltpu.get_barrier_semaphore()
    for step in range(1, n):
        pl.semaphore_signal(barrier, inc=1, device_id={"tm": lax.rem(me + step, n)}, device_id_type=MESH)

    def initial_at(z):
        return jnp.concatenate(
            [init_ref[pl.ds(z * inst + i, reps, stride=zones * inst), :] for i in range(inst)], axis=0
        )

    def forcing_at(slot, z):
        return jnp.concatenate(
            [forc_ref[pl.ds((i * reps * zones + z) * M + slot, reps, stride=zones * M), :] for i in range(inst)],
            axis=0,
        )

    def emit_out(slot, z, value):
        for i in range(inst):
            out_ref[pl.ds((i * reps * zones + z) * M + slot, reps, stride=zones * M), :] = value[
                i * reps : (i + 1) * reps
            ]

    row = lax.broadcasted_iota(jnp.int32, (rows, blk), 0)

    def put(dst, z, value):
        def write(slot, v):
            high = v.astype(jnp.bfloat16)
            low = (v - high.astype(jnp.float32)).astype(jnp.bfloat16)
            x[dst, slot, :rows] = high
            x[dst, slot, rows:] = low

        write(z + 1, value)
        if z == 0:
            rolled = pltpu.roll(value, rows - 1, 0)
            write(zones + 1, jnp.where(row % reps == reps - 1, 0.0, rolled))
        if z == zones - 1:
            rolled = pltpu.roll(value, 1, 0)
            write(0, jnp.where(row % reps == 0, 0.0, rolled))

    def propagate(src, which, delta_t, emit):
        for z in range(zones):
            left = jnp.concatenate([x[src, z + k] for k in range(3)], axis=1)
            acc = jnp.dot(left, weights[which, z], preferred_element_type=jnp.float32)
            mixing = (acc[:rows, :blk] + acc[:rows, blk:]) + (acc[rows:, :blk] + acc[rows:, blk:])
            emit(z, newton(mixing, delta_t))

    def prepare(which):
        @pl.loop(0, pieces)
        def _(c):
            load(which, c).wait()
            if which == 0:

                @pl.when(c == pieces - 1)
                def _():
                    for later in range(pieces):
                        load(1, later).start()

            for zz in range(part):
                z = c * part + zz
                for k in range(3):
                    turned = raw[which, z, k].T
                    high = turned.astype(jnp.bfloat16)
                    weights[which, z, k * blk : (k + 1) * blk, :blk] = high
                    weights[which, z, k * blk : (k + 1) * blk, blk:] = (
                        turned - high.astype(jnp.float32)
                    ).astype(jnp.bfloat16)

    def fine_step(t, src, sink, keep=True):
        def emit(z, s):
            value = s + forcing_at(t, z)
            if keep:
                put(1 - src, z, value)
            sink(z, value)

        propagate(src, 0, DELTA, emit)

    def store_to(buf):
        def emit(z, value):
            buf[z] = value

        return emit

    def drop(z, value):
        pass

    prepare(0)
    for copy in state_loads:
        copy.wait()

    @pl.when(me == 0)
    def _():
        for z in range(zones):
            put(0, z, initial_at(z))
        fine_step(0, 0, drop)

    @pl.when(me > 0)
    def _():
        for z in range(zones):
            put(1, z, forcing_at(0, z))

    for t in range(1, M):
        fine_step(t, t % 2, store_to(ubuf) if t == M - 1 else drop, keep=t < M - 1)
    pl.semaphore_wait(barrier, n - 1)

    onward = pltpu.make_async_remote_copy(
        src_ref=ubuf, dst_ref=carr, send_sem=carr_send, recv_sem=carr_recv,
        device_id={"tm": lax.rem(me + 1, n)}, device_id_type=MESH,
    )

    @pl.when(me < n - 1)
    def _():
        onward.start()

    prepare(1)
    for z in range(zones):
        put(0, z, initial_at(z))
    propagate(0, 1, coarse_dt, store_to(pbuf))

    @pl.when(me == 0)
    def _():
        for z in range(zones):
            rbuf[0, z] = ubuf[z] - pbuf[z]

    @pl.when(me > 0)
    def _():
        onward.wait_recv()
        for z in range(zones):
            put(0, z, carr[z])
        propagate(0, 1, coarse_dt, store_to(qbuf))
        for t in range(M - 1):
            fine_step(t, t % 2, drop)

        def right_side(z, value):
            rbuf[me, z] = value - qbuf[z]

        fine_step(M - 1, (M - 1) % 2, right_side, keep=False)

    def share(target):
        return pltpu.make_async_remote_copy(
            src_ref=rbuf.at[me], dst_ref=rbuf.at[me], send_sem=r_send.at[target], recv_sem=r_recv.at[me],
            device_id={"tm": target}, device_id_type=MESH,
        )

    def forward(j):
        return pltpu.make_async_remote_copy(
            src_ref=rbuf.at[j], dst_ref=rbuf.at[j], send_sem=fwd_send.at[j], recv_sem=r_recv.at[j],
            device_id={"tm": lax.rem(me + n - 1, n)}, device_id_type=MESH,
        )

    for target in range(n - 1, 0, -2):

        @pl.when(me < target)
        def _():
            share(target).start()

    def chain(j, _):
        forward(j).wait_recv()

        @pl.when(jnp.logical_and(odd == 1, j < me - 1))
        def _():
            forward(j).start()

        for z in range(zones):
            put(0, z, pbuf[z] + rbuf[j, z])
        propagate(0, 1, coarse_dt, store_to(pbuf))
        return 0

    lax.fori_loop(0, me, chain, 0)
    for z in range(zones):
        emit_out(M - 1, z, pbuf[z] + rbuf[me, z])
    for t in range(M - 1):
        fine_step(t, t % 2, functools.partial(emit_out, t), keep=t < M - 2)

    @pl.when(me < n - 1)
    def _():
        onward.wait_send()

    for target in range(n - 1, 0, -2):

        @pl.when(me < target)
        def _():
            share(target).wait_send()

    def drain(j, _):
        forward(j).wait_send()
        return 0

    lax.fori_loop(0, jnp.where(odd == 1, me - 1, 0), drain, 0)


def solution(mesh):
    n = mesh.shape["tm"]

    def body(initial, forcing, fine_blocks, coarse_blocks):
        inst, slots, cells = forcing.shape
        zones, _, blk, _ = fine_blocks.shape
        blocks = cells // blk
        reps = blocks // zones
        rows = inst * reps
        assert slots == M and n % 2 == 0
        pieces = 4 if zones % 4 == 0 else 1
        init_rows = initial.reshape(inst, blocks, blk).transpose(1, 0, 2).reshape(-1, blk)
        forc_rows = forcing.reshape(inst, slots, blocks, blk).transpose(0, 2, 1, 3).reshape(-1, blk)
        state = pltpu.VMEM((zones, rows, blk), jnp.float32)
        out = pl.pallas_call(
            functools.partial(kernel, n, inst, zones, reps, pieces),
            out_shape=pltpu.VMEM(forc_rows.shape, jnp.float32),
            in_specs=[pl.BlockSpec(memory_space=pltpu.HBM)] * 4,
            out_specs=pl.BlockSpec(memory_space=pltpu.VMEM),
            scratch_shapes=[
                pltpu.VMEM(init_rows.shape, jnp.float32),
                pltpu.VMEM(forc_rows.shape, jnp.float32),
                pltpu.VMEM((2,) + fine_blocks.shape, jnp.float32),
                pltpu.VMEM((2, zones, 3 * blk, 2 * blk), jnp.bfloat16),
                pltpu.VMEM((2, zones + 2, 2 * rows, blk), jnp.bfloat16),
                state,
                state,
                pltpu.VMEM((n, zones, rows, blk), jnp.float32),
                state,
                state,
                pltpu.SemaphoreType.DMA((2, pieces)),
                pltpu.SemaphoreType.DMA((2,)),
                pltpu.SemaphoreType.DMA,
                pltpu.SemaphoreType.DMA,
                pltpu.SemaphoreType.DMA((n,)),
                pltpu.SemaphoreType.DMA((n,)),
                pltpu.SemaphoreType.DMA((n,)),
            ],
            compiler_params=pltpu.CompilerParams(collective_id=0, has_side_effects=True),
        )(init_rows, forc_rows, fine_blocks, coarse_blocks)
        return out.reshape(inst, blocks, slots, blk).transpose(0, 2, 1, 3).reshape(forcing.shape)

    in_specs = (P("grp", None), P("grp", "tm", None), P(), P())
    out_specs = P("grp", "tm", None)
    return jax.shard_map(body, mesh=mesh, in_specs=in_specs, out_specs=out_specs, check_vma=False)
```

```python
import functools

import jax
import jax.numpy as jnp
from jax import lax
from jax.experimental import pallas as pl
from jax.experimental.pallas import tpu as pltpu
from jax.sharding import PartitionSpec as P

M = 4
DELTA = 0.05
MESH = pl.DeviceIdType.MESH


def newton(mixing, delta_t):
    solved = mixing
    for _ in range(2):
        squared = solved * solved
        solved = (mixing + (2.0 * delta_t) * solved * squared) / (
            (1.0 - delta_t) + (3.0 * delta_t) * squared
        )
    return solved


def kernel(
    n, inst, zones, reps, pieces,
    init_hbm, forc_hbm, fine_hbm, coarse_hbm, out_ref,
    init_ref, forc_ref, raw, weights, x, ubuf, carr, rbuf, pbuf, qbuf,
    load_sem, state_sem, carr_send, carr_recv, r_send, r_recv, fwd_send,
):
    me = lax.axis_index("tm")
    blk = raw.shape[-1]
    rows = inst * reps
    coarse_dt = DELTA * M
    part = zones // pieces
    odd = lax.rem(me, 2)

    def load(which, c):
        span = pl.ds(c * part, part)
        return pltpu.make_async_copy((fine_hbm, coarse_hbm)[which].at[span], raw.at[which, span], load_sem.at[which, c])

    state_loads = [
        pltpu.make_async_copy(init_hbm, init_ref, state_sem.at[0]),
        pltpu.make_async_copy(forc_hbm, forc_ref, state_sem.at[1]),
    ]
    for c in range(pieces):
        load(0, c).start()
    for copy in state_loads:
        copy.start()

    barrier = pltpu.get_barrier_semaphore()
    for step in range(1, n):
        pl.semaphore_signal(barrier, inc=1, device_id={"tm": lax.rem(me + step, n)}, device_id_type=MESH)

    def initial_at(z):
        return jnp.concatenate(
            [init_ref[pl.ds(z * inst + i, reps, stride=zones * inst), :] for i in range(inst)], axis=0
        )

    def forcing_at(slot, z):
        return jnp.concatenate(
            [forc_ref[pl.ds((i * reps * zones + z) * M + slot, reps, stride=zones * M), :] for i in range(inst)],
            axis=0,
        )

    def emit_out(slot, z, value):
        for i in range(inst):
            out_ref[pl.ds((i * reps * zones + z) * M + slot, reps, stride=zones * M), :] = value[
                i * reps : (i + 1) * reps
            ]

    row = lax.broadcasted_iota(jnp.int32, (rows, blk), 0)

    def put(dst, z, value):
        def write(slot, v):
            high = v.astype(jnp.bfloat16)
            low = (v - high.astype(jnp.float32)).astype(jnp.bfloat16)
            x[dst, slot, :rows] = high
            x[dst, slot, rows:] = low

        write(z + 1, value)
        if z == 0:
            rolled = pltpu.roll(value, rows - 1, 0)
            write(zones + 1, jnp.where(row % reps == reps - 1, 0.0, rolled))
        if z == zones - 1:
            rolled = pltpu.roll(value, 1, 0)
            write(0, jnp.where(row % reps == 0, 0.0, rolled))

    def propagate(src, which, delta_t, emit):
        for z in range(zones):
            left = jnp.concatenate([x[src, z + k] for k in range(3)], axis=1)
            acc = jnp.dot(left, weights[which, z], preferred_element_type=jnp.float32)
            mixing = (acc[:rows, :blk] + acc[:rows, blk:]) + (acc[rows:, :blk] + acc[rows:, blk:])
            emit(z, newton(mixing, delta_t))

    def prepare(which):
        @pl.loop(0, pieces)
        def _(c):
            load(which, c).wait()
            if which == 0:

                @pl.when(c == pieces - 1)
                def _():
                    for later in range(pieces):
                        load(1, later).start()

            for zz in range(part):
                z = c * part + zz
                for k in range(3):
                    turned = raw[which, z, k].T
                    high = turned.astype(jnp.bfloat16)
                    weights[which, z, k * blk : (k + 1) * blk, :blk] = high
                    weights[which, z, k * blk : (k + 1) * blk, blk:] = (
                        turned - high.astype(jnp.float32)
                    ).astype(jnp.bfloat16)

    def fine_step(t, src, sink, keep=True):
        def emit(z, s):
            value = s + forcing_at(t, z)
            if keep:
                put(1 - src, z, value)
            sink(z, value)

        propagate(src, 0, DELTA, emit)

    def store_to(buf):
        def emit(z, value):
            buf[z] = value

        return emit

    def drop(z, value):
        pass

    prepare(0)
    for copy in state_loads:
        copy.wait()

    @pl.when(me == 0)
    def _():
        for z in range(zones):
            put(0, z, initial_at(z))
        fine_step(0, 0, drop)

    @pl.when(me > 0)
    def _():
        for z in range(zones):
            put(1, z, forcing_at(0, z))

    for t in range(1, M):
        fine_step(t, t % 2, store_to(ubuf) if t == M - 1 else drop, keep=t < M - 1)
    pl.semaphore_wait(barrier, n - 1)

    onward = pltpu.make_async_remote_copy(
        src_ref=ubuf, dst_ref=carr, send_sem=carr_send, recv_sem=carr_recv,
        device_id={"tm": lax.rem(me + 1, n)}, device_id_type=MESH,
    )

    @pl.when(me < n - 1)
    def _():
        onward.start()

    prepare(1)
    for z in range(zones):
        put(0, z, initial_at(z))
    propagate(0, 1, coarse_dt, store_to(pbuf))

    @pl.when(me == 0)
    def _():
        for z in range(zones):
            rbuf[0, z] = ubuf[z] - pbuf[z]

    @pl.when(me > 0)
    def _():
        onward.wait_recv()
        for z in range(zones):
            put(0, z, carr[z])
        propagate(0, 1, coarse_dt, store_to(qbuf))
        for t in range(M - 1):
            fine_step(t, t % 2, drop)

        def right_side(z, value):
            rbuf[me, z] = value - qbuf[z]

        fine_step(M - 1, (M - 1) % 2, right_side, keep=False)

    def share(target):
        return pltpu.make_async_remote_copy(
            src_ref=rbuf.at[me], dst_ref=rbuf.at[me], send_sem=r_send.at[target], recv_sem=r_recv.at[me],
            device_id={"tm": target}, device_id_type=MESH,
        )

    def forward(j):
        return pltpu.make_async_remote_copy(
            src_ref=rbuf.at[j], dst_ref=rbuf.at[j], send_sem=fwd_send.at[j], recv_sem=r_recv.at[j],
            device_id={"tm": lax.rem(me + n - 1, n)}, device_id_type=MESH,
        )

    for target in range(n - 1, 0, -2):

        @pl.when(me < target)
        def _():
            share(target).start()

    def chain(j, _):
        forward(j).wait_recv()

        @pl.when(jnp.logical_and(odd == 1, j < me - 1))
        def _():
            forward(j).start()

        for z in range(zones):
            put(0, z, pbuf[z] + rbuf[j, z])
        propagate(0, 1, coarse_dt, store_to(pbuf))
        return 0

    lax.fori_loop(0, me, chain, 0)
    for z in range(zones):
        emit_out(M - 1, z, pbuf[z] + rbuf[me, z])
    for t in range(M - 1):
        fine_step(t, t % 2, functools.partial(emit_out, t), keep=t < M - 2)

    @pl.when(me < n - 1)
    def _():
        onward.wait_send()

    for target in range(n - 1, 0, -2):

        @pl.when(me < target)
        def _():
            share(target).wait_send()

    def drain(j, _):
        forward(j).wait_send()
        return 0

    lax.fori_loop(0, jnp.where(odd == 1, me - 1, 0), drain, 0)


def solution(mesh):
    n = mesh.shape["tm"]

    def body(initial, forcing, fine_blocks, coarse_blocks):
        inst, slots, cells = forcing.shape
        zones, _, blk, _ = fine_blocks.shape
        blocks = cells // blk
        reps = blocks // zones
        rows = inst * reps
        assert slots == M and n % 2 == 0
        pieces = 8 if zones % 8 == 0 else 1
        init_rows = initial.reshape(inst, blocks, blk).transpose(1, 0, 2).reshape(-1, blk)
        forc_rows = forcing.reshape(inst, slots, blocks, blk).transpose(0, 2, 1, 3).reshape(-1, blk)
        state = pltpu.VMEM((zones, rows, blk), jnp.float32)
        out = pl.pallas_call(
            functools.partial(kernel, n, inst, zones, reps, pieces),
            out_shape=pltpu.VMEM(forc_rows.shape, jnp.float32),
            in_specs=[pl.BlockSpec(memory_space=pltpu.HBM)] * 4,
            out_specs=pl.BlockSpec(memory_space=pltpu.VMEM),
            scratch_shapes=[
                pltpu.VMEM(init_rows.shape, jnp.float32),
                pltpu.VMEM(forc_rows.shape, jnp.float32),
                pltpu.VMEM((2,) + fine_blocks.shape, jnp.float32),
                pltpu.VMEM((2, zones, 3 * blk, 2 * blk), jnp.bfloat16),
                pltpu.VMEM((2, zones + 2, 2 * rows, blk), jnp.bfloat16),
                state,
                state,
                pltpu.VMEM((n, zones, rows, blk), jnp.float32),
                state,
                state,
                pltpu.SemaphoreType.DMA((2, pieces)),
                pltpu.SemaphoreType.DMA((2,)),
                pltpu.SemaphoreType.DMA,
                pltpu.SemaphoreType.DMA,
                pltpu.SemaphoreType.DMA((n,)),
                pltpu.SemaphoreType.DMA((n,)),
                pltpu.SemaphoreType.DMA((n,)),
            ],
            compiler_params=pltpu.CompilerParams(collective_id=0, has_side_effects=True),
        )(init_rows, forc_rows, fine_blocks, coarse_blocks)
        return out.reshape(inst, blocks, slots, blk).transpose(0, 2, 1, 3).reshape(forcing.shape)

    in_specs = (P("grp", None), P("grp", "tm", None), P(), P())
    out_specs = P("grp", "tm", None)
    return jax.shard_map(body, mesh=mesh, in_specs=in_specs, out_specs=out_specs, check_vma=False)
```
